8 devices in a mesh: fsdp: 8 (over z, y, x, core).
Axes of the slice: x: 2, y: 2, z: 1, core: 2. Of those that a mesh axis runs over, the one named last changes fastest.
Arguments:
- tok_ids: int32 [16, 1024], P('fsdp')
- grad_out: bfloat16 [16, 1024, 1536], P('fsdp')
- emb_table: bfloat16 [151936, 1536], P('fsdp')
- norm_gain: bfloat16 [1536], P('fsdp')
- w_query: bfloat16 [1536, 1536], P('fsdp')
- b_query: bfloat16 [1536], P('fsdp')
- w_key: bfloat16 [1536, 256], P('fsdp')
- b_key: bfloat16 [256], P('fsdp')
- w_value: bfloat16 [1536, 256], P('fsdp')
- b_value: bfloat16 [256], P('fsdp')
- w_out: bfloat16 [1536, 1536], P('fsdp')
Outputs:
- output 1: bfloat16 [16, 1024, 1536], P('fsdp')
- output 2: bfloat16 [151936, 1536], P('fsdp')
- output 3: float32 [1536], P('fsdp')
- output 4: float32 [1536, 1536], P('fsdp')
- output 5: float32 [1536], P('fsdp')
- output 6: float32 [1536, 256], P('fsdp')
- output 7: float32 [256], P('fsdp')
- output 8: float32 [1536, 256], P('fsdp')
- output 9: float32 [256], P('fsdp')
- output 10: float32 [1536, 1536], P('fsdp')
All inputs are finite; a program needn't handle non-finite values.
Results may differ from the reference program's by a relative error of at most 0.0157803.
Values are sent between devices in bfloat16 or wider.
A program may use at most 1 GiB of HBM per device.

```python
import jax
import jax.numpy as jnp
from jax import lax

VOCAB = 151936
D_MODEL = 1536
HEADS = 12
KV_HEADS = 2
HEAD_DIM = 128
BATCH = 16
SEQ = 1024
HOT_IDS = 4096
ROPE_THETA = 1.0e6
NORM_EPS = 1e-6
MASK_VALUE = -1e30


def draw_ids(key_ids):
    key_pick, key_hot, key_wide = jax.random.split(key_ids, 3)
    pick_hot = jax.random.randint(key_pick, (BATCH, SEQ), 0, 2)
    low_ids = jax.random.randint(key_hot, (BATCH, SEQ), 0, HOT_IDS)
    hot_ids = (low_ids * low_ids) // HOT_IDS
    wide_ids = jax.random.randint(key_wide, (BATCH, SEQ), 0, VOCAB)
    tok_ids = jnp.where(pick_hot == 0, hot_ids, wide_ids).astype(jnp.int32)
    return tok_ids.at[0, SEQ - 1].set(VOCAB - 1)


def setup_inputs(seed: int = 0) -> dict:
    key_list = jax.random.split(jax.random.key(seed), 12)
    q_width = HEADS * HEAD_DIM
    kv_width = KV_HEADS * HEAD_DIM
    in_scale = D_MODEL ** -0.5
    out_scale = q_width ** -0.5

    def normal(key_n, shape):
        return jax.random.normal(key_n, shape, jnp.float32)

    return {
        "tok_ids": draw_ids(key_list[0]),
        "grad_out": normal(key_list[1], (BATCH, SEQ, D_MODEL)).astype(jnp.bfloat16),
        "emb_table": normal(key_list[2], (VOCAB, D_MODEL)).astype(jnp.bfloat16),
        "norm_gain": (1.0 + 0.3 * normal(key_list[3], (D_MODEL,))).astype(jnp.bfloat16),
        "w_query": (in_scale * normal(key_list[4], (D_MODEL, q_width))).astype(jnp.bfloat16),
        "b_query": (0.5 * normal(key_list[5], (q_width,))).astype(jnp.bfloat16),
        "w_key": (in_scale * normal(key_list[6], (D_MODEL, kv_width))).astype(jnp.bfloat16),
        "b_key": (0.5 * normal(key_list[7], (kv_width,))).astype(jnp.bfloat16),
        "w_value": (in_scale * normal(key_list[8], (D_MODEL, kv_width))).astype(jnp.bfloat16),
        "b_value": (0.5 * normal(key_list[9], (kv_width,))).astype(jnp.bfloat16),
        "w_out": (out_scale * normal(key_list[10], (q_width, D_MODEL))).astype(jnp.bfloat16),
    }


def rope_tables():
    half_dim = HEAD_DIM // 2
    inv_freq = jnp.power(ROPE_THETA, -(jnp.arange(half_dim, dtype=jnp.float32) * 2.0 / HEAD_DIM))
    angles = jnp.arange(SEQ, dtype=jnp.float32)[:, None] * inv_freq[None, :]
    angles = jnp.concatenate([angles, angles], axis=-1)
    return jnp.cos(angles)[:, None, :], jnp.sin(angles)[:, None, :]


def rotate(vector, cos_t, sin_t):
    half_dim = HEAD_DIM // 2
    turned = jnp.concatenate([-vector[..., half_dim:], vector[..., :half_dim]], axis=-1)
    return vector * cos_t + turned * sin_t


def block_seq(x_seq, params):
    gain_vec, w_query, b_query, w_key, b_key, w_value, b_value, w_out = params
    cos_t, sin_t = rope_tables()
    q_group = HEADS // KV_HEADS
    inv_rms = lax.rsqrt(jnp.mean(x_seq * x_seq, axis=-1, keepdims=True) + NORM_EPS)
    hidden = (x_seq * inv_rms * gain_vec).astype(jnp.bfloat16).astype(jnp.float32)
    q_lin = jnp.dot(hidden, w_query, preferred_element_type=jnp.float32) + b_query
    k_lin = jnp.dot(hidden, w_key, preferred_element_type=jnp.float32) + b_key
    v_lin = jnp.dot(hidden, w_value, preferred_element_type=jnp.float32) + b_value
    q_rot = rotate(q_lin.reshape(SEQ, HEADS, HEAD_DIM), cos_t, sin_t)
    q_rot = q_rot.astype(jnp.bfloat16).astype(jnp.float32).reshape(SEQ, KV_HEADS, q_group, HEAD_DIM)
    k_rot = rotate(k_lin.reshape(SEQ, KV_HEADS, HEAD_DIM), cos_t, sin_t)
    k_rot = k_rot.astype(jnp.bfloat16).astype(jnp.float32)
    v_val = v_lin.reshape(SEQ, KV_HEADS, HEAD_DIM).astype(jnp.bfloat16).astype(jnp.float32)
    scores = jnp.einsum("qkgd,skd->kgqs", q_rot, k_rot) * (HEAD_DIM ** -0.5)
    causal = jnp.arange(SEQ)[:, None] >= jnp.arange(SEQ)[None, :]
    scores = jnp.where(causal, scores, MASK_VALUE)
    prob_b = jax.nn.softmax(scores, axis=-1).astype(jnp.bfloat16).astype(jnp.float32)
    attn_out = jnp.einsum("kgqs,skd->qkgd", prob_b, v_val).reshape(SEQ, HEADS * HEAD_DIM)
    attn_out = attn_out.astype(jnp.bfloat16).astype(jnp.float32)
    proj_out = jnp.dot(attn_out, w_out, preferred_element_type=jnp.float32)
    return (x_seq + proj_out).astype(jnp.bfloat16)


def reference(tok_ids, grad_out, emb_table, norm_gain, w_query, b_query, w_key, b_key, w_value, b_value, w_out):
    x_all = jnp.take(emb_table, tok_ids, axis=0).astype(jnp.float32)
    params = tuple(weight.astype(jnp.float32) for weight in (norm_gain, w_query, b_query, w_key, b_key, w_value, b_value, w_out))
    seq_step = jax.checkpoint(block_seq)

    def forward(x_in, prm_list):
        return lax.map(lambda x_seq: seq_step(x_seq, prm_list), x_in)

    block_out, pullback = jax.vjp(forward, x_all, params)
    d_x, d_params = pullback(grad_out)
    grad_table = jax.ops.segment_sum(d_x.reshape(-1, D_MODEL), tok_ids.reshape(-1), num_segments=VOCAB)
    grad_table = grad_table.astype(jnp.bfloat16)
    return (block_out, grad_table, d_params[0], d_params[1], d_params[2], d_params[3], d_params[4], d_params[5], d_params[6], d_params[7])
```

```python
import functools

import jax
import jax.numpy as jnp
from jax import lax
from jax.experimental import pallas as pl
from jax.experimental.pallas import tpu as pltpu
from jax.sharding import PartitionSpec as P

F32 = jnp.float32
BF16 = jnp.bfloat16
I32 = jnp.int32
MESH = pl.DeviceIdType.MESH

LANE = 128
SUB = 8
HEAD_DIM = LANE
ROPE_THETA = 1.0e6
NORM_EPS = 1e-6
MASK_VALUE = -1e30

N_DEV = 8
SEQ = 1024
SEQS = 2
TOK = SEQ * SEQS
D = 1536
HEADS = 12
KV = 2
GROUP = HEADS // KV
ROWS = 18992
HOT = 4096
CAP = 176
COLD = N_DEV * CAP
BUF = HOT + COLD
QKV = D + 2 * KV * HEAD_DIM
VMEM_MAX = 66_000_000


def params(**kw):
    return pltpu.CompilerParams(vmem_limit_bytes=VMEM_MAX, **kw)


ANY = pl.BlockSpec(memory_space=pl.ANY)


def full(*shape):
    return pl.BlockSpec(shape, lambda *i: (0,) * len(shape))


def by_row(*shape):
    return pl.BlockSpec(shape, lambda i, *_: (i,) + (0,) * (len(shape) - 1))


def shape_of(dtype, *shape):
    return jax.ShapeDtypeStruct(shape, dtype)


def row_sum(v):
    return jnp.sum(v, axis=-1, keepdims=True)


def row_mean(v):
    return jnp.mean(v, axis=-1, keepdims=True)


def col_sum(v):
    return jnp.sum(v, axis=0, keepdims=True)


def iota(dtype, shape, dim):
    return lax.broadcasted_iota(I32, shape, dim).astype(dtype)


def cost(flops, nbytes):
    return pl.CostEstimate(flops=int(flops), bytes_accessed=int(nbytes), transcendentals=0)


def dot(a, b, dims):
    return lax.dot_general(a, b, (dims, ((), ())), preferred_element_type=F32)


NN = ((1,), (0,))
NT = ((1,), (1,))
TN = ((0,), (0,))


def index_kernel(me_ref, mine_ref, ids_ref, xi_ref, own_ref, ovf_ref, rank_ref):
    me = me_ref[0]
    r_io = lax.broadcasted_iota(I32, (LANE, LANE), 0)
    c_io = lax.broadcasted_iota(I32, (LANE, LANE), 1)
    own_s = lax.broadcasted_iota(I32, (8, 1), 0)
    lo_s = jnp.maximum(own_s * ROWS, HOT).astype(F32)
    hi_s = (own_s * ROWS + ROWS).astype(F32)
    up = (r_io < c_io).astype(BF16)
    run = jnp.zeros((8, 1), F32)
    for b in range(TOK // LANE):
        blk = mine_ref[:, b * LANE : (b + 1) * LANE]
        hit = jnp.logical_and(blk >= lo_s, blk < hi_s)
        one = hit.astype(F32)
        rank = dot(one.astype(BF16), up, NN) + run
        run = run + row_sum(one)
        slot = jnp.minimum(rank, CAP - 1) + own_s.astype(F32) * CAP + HOT
        pick = col_sum(jnp.where(hit, slot, 0.0))
        xi_ref[b : b + 1, :] = jnp.where(blk < HOT, blk, pick).astype(I32)
    lane = lax.broadcasted_iota(I32, (1, 64), 1)
    own_l = lax.rem(lane, 8)
    lo_l = jnp.maximum(own_l * ROWS, HOT).astype(F32)
    hi_l = (own_l * ROWS + ROWS).astype(F32)
    low = (r_io > c_io).astype(BF16)
    run = jnp.zeros((1, 64), F32)
    for b in range(TOK // LANE):
        blk = ids_ref[b * LANE : (b + 1) * LANE, :]
        hit = jnp.logical_and(blk >= lo_l, blk < hi_l)
        one = hit.astype(F32)
        rank = dot(low, one.astype(BF16), NN) + run
        run = run + col_sum(one)
        rank_ref[b * LANE : (b + 1) * LANE, :] = jnp.where(hit, rank, -1.0)
    ovf_ref[...] = jnp.broadcast_to(jnp.max(run, axis=1, keepdims=True), ovf_ref.shape)
    slot_io = lax.broadcasted_iota(I32, (1, 256), 1).astype(F32)
    first = (me * ROWS).astype(F32)
    for s in range(N_DEV):
        col = lane == s * 8 + me
        acc = jnp.zeros((8, 256), F32)
        for b in range(TOK // 256):
            rk = rank_ref[b * 256 : (b + 1) * 256, :]
            idb = ids_ref[b * 256 : (b + 1) * 256, :]
            rk1 = row_sum(jnp.where(col, rk, 0.0))
            loc = row_sum(jnp.where(col, idb, 0.0)) - first + 1.0
            hitv = jnp.where(rk1 == slot_io, loc, 0.0)
            acc = acc + jnp.sum(hitv.reshape(32, 8, 256), axis=0)
        own_ref[s : s + 1, :] = col_sum(acc).astype(I32) - 1


def index_maps(me, mine, ids64):
    return pl.pallas_call(
        index_kernel,
        grid_spec=pltpu.PrefetchScalarGridSpec(
            num_scalar_prefetch=1,
            grid=(1,),
            in_specs=[full(1, TOK), full(TOK, 64)],
            out_specs=[
                full(TOK // LANE, LANE),
                full(8, 256),
                full(8, LANE),
            ],
            scratch_shapes=[pltpu.VMEM((TOK, 64), F32)],
        ),
        out_shape=[
            shape_of(I32, TOK // LANE, LANE),
            shape_of(I32, 8, 256),
            shape_of(F32, 8, LANE),
        ],
        compiler_params=params(),
        cost_estimate=cost(5e9, 2e6),
        name="index_maps",
    )(me, mine, ids64)


def merge_kernel(row_ref, col_ref, tgt_ref, rep_ref):
    n = row_ref.shape[1]
    for b in range(n // LANE):
        row = row_ref[:, b * LANE : (b + 1) * LANE]
        pair = jnp.floor(row * 0.5)
        best = jnp.full((8, LANE), float(n), F32)
        for c in range(n // LANE):
            other = jnp.floor(col_ref[c * LANE : (c + 1) * LANE, :] * 0.5)
            kk = (lax.broadcasted_iota(I32, (LANE, 1), 0) + c * LANE).astype(F32)
            hit = jnp.where(other == pair, kk, float(n))
            best = jnp.minimum(best, jnp.min(hit.reshape(16, 8, LANE), axis=0))
        rep = jnp.min(best, axis=0, keepdims=True)
        par = row - 2.0 * pair
        tgt_ref[b : b + 1, :] = (2.0 * rep + par).astype(I32)
        rep_ref[b : b + 1, :] = rep.astype(I32)


def merge_maps(row, col):
    n = row.shape[1]
    return pl.pallas_call(
        merge_kernel,
        out_shape=[shape_of(I32, n // LANE, LANE)] * 2,
        compiler_params=params(),
        cost_estimate=cost(5e9, 1e6),
        name="merge_maps",
    )(row, col)


def gather_kernel(n, idx_s, idx_ref, src_ref, out_ref, buf, sem):
    i = pl.program_id(0)

    def fetch(blk, slot):
        def body(q, c):
            for u in range(8):
                j = q * 8 + u
                r = lax.shift_right_logical(jnp.maximum(idx_s[blk, j], 0), 1)
                pltpu.make_async_copy(
                    src_ref.at[pl.ds(pl.multiple_of(r * 2, 2), 2), :],
                    buf.at[slot, pl.ds(pl.multiple_of(j * 2, 2), 2), :],
                    sem.at[slot],
                ).start()
            return c

        lax.fori_loop(0, n // 8, body, 0)

    slot = lax.rem(i, 2)

    @pl.when(i == 0)
    def _():
        fetch(0, 0)

    @pl.when(i + 1 < pl.num_programs(0))
    def _():
        fetch(i + 1, 1 - slot)

    idx = jnp.maximum(idx_ref[pl.ds(i, 1), :][:, :n], 0)
    k_io = lax.broadcasted_iota(I32, (2 * n, n), 0)
    j_io = lax.broadcasted_iota(I32, (2 * n, n), 1)
    want = 2 * j_io + jnp.bitwise_and(idx, 1)
    pick = (k_io == want).astype(BF16)
    pltpu.make_async_copy(src_ref.at[pl.ds(0, 2 * n), :], buf.at[slot], sem.at[slot]).wait()
    out_ref[0] = dot(pick, buf[slot], TN).astype(BF16)


def gather_rows(src, idx, n):
    blocks = idx.shape[0]
    return pl.pallas_call(
        functools.partial(gather_kernel, n),
        grid_spec=pltpu.PrefetchScalarGridSpec(
            num_scalar_prefetch=1,
            grid=(blocks,),
            in_specs=[full(*idx.shape), ANY],
            out_specs=by_row(1, n, D),
            scratch_shapes=[pltpu.VMEM((2, 2 * n, D), BF16), pltpu.SemaphoreType.DMA((2,))],
        ),
        out_shape=shape_of(BF16, blocks, n, D),
        compiler_params=params(),
        cost_estimate=cost(2e10, blocks * n * D * 6),
        name="gather_rows",
    )(idx, idx, src)


CHUNKS = 8
HALF = HOT // 2
CH = HALF // CHUNKS


def lookup_kernel(table, send, buf, stage, ld_sem, st_sem, a_send, a_recv, b_send, b_recv, d_send, d_recv, c_send, c_recv):
    me = lax.axis_index("fsdp")
    barrier = pltpu.get_barrier_semaphore()
    for off in range(1, N_DEV):
        pl.semaphore_signal(barrier, inc=1, device_id=(lax.rem(me + off, N_DEV),), device_id_type=MESH)
    pl.semaphore_wait(barrier, N_DEV - 1)

    def a_rows(k):
        return pl.ds(k * CH, CH)

    def b_rows(k):
        return pl.ds(HALF + k * CH, CH)

    def remote(src, rows, s_sem, r_sem, dev):
        return pltpu.make_async_remote_copy(src_ref=src.at[rows, :], dst_ref=buf.at[rows, :], send_sem=s_sem, recv_sem=r_sem, device_id=(dev,), device_id_type=MESH)

    def cold(off):
        dst = lax.rem(me + off, N_DEV)
        return pltpu.make_async_remote_copy(
            src_ref=send.at[dst],
            dst_ref=buf.at[pl.ds(pl.multiple_of(HOT + me * CAP, 16), CAP), :],
            send_sem=c_send.at[off],
            recv_sem=c_recv.at[off],
            device_id=(dst,),
            device_id_type=MESH,
        )

    def cold_in(off):
        src = lax.rem(me - off + N_DEV, N_DEV)
        return pltpu.make_async_remote_copy(
            src_ref=send.at[0],
            dst_ref=buf.at[pl.ds(pl.multiple_of(HOT + src * CAP, 16), CAP), :],
            send_sem=c_send.at[off],
            recv_sem=c_recv.at[off],
            device_id=(src,),
            device_id_type=MESH,
        )

    root = me == 0
    nxt = {2: 6, 6: 4, 1: 5, 5: 7, 7: 3}
    for k in range(CHUNKS):

        @pl.when(root)
        def _(k=k):
            remote(table, a_rows(k), a_send.at[k], a_recv.at[k], 2).start()
            remote(table, b_rows(k), b_send.at[k], b_recv.at[k], 1).start()
            remote(table, a_rows(k), d_send.at[k], d_recv.at[k], 1).start()

        for dev in (2, 6, 4):

            @pl.when(me == dev)
            def _(k=k, dev=dev):
                remote(table, a_rows(k), a_send.at[k], a_recv.at[k], 0).wait_recv()
                if dev in nxt:
                    remote(buf, a_rows(k), a_send.at[k], a_recv.at[k], nxt[dev]).start()
                remote(buf, a_rows(k), d_send.at[k], d_recv.at[k], dev + 1).start()

        for dev in (1, 5, 7, 3):

            @pl.when(me == dev)
            def _(k=k, dev=dev):
                remote(table, b_rows(k), b_send.at[k], b_recv.at[k], 0).wait_recv()
                if dev in nxt:
                    remote(buf, b_rows(k), b_send.at[k], b_recv.at[k], nxt[dev]).start()
                if dev != 1:
                    remote(buf, b_rows(k), d_send.at[k], d_recv.at[k], dev - 1).start()

        if 1 <= k + 1 < N_DEV:
            cold(k + 1).start()

    ld = pltpu.make_async_copy(send.at[me], stage.at[pl.ds(0, CAP), :], ld_sem)
    ld.start()
    ld.wait()
    st = pltpu.make_async_copy(stage.at[pl.ds(0, CAP), :], buf.at[pl.ds(pl.multiple_of(HOT + me * CAP, 16), CAP), :], st_sem)
    st.start()
    st.wait()

    @pl.when(root)
    def _():
        big = pltpu.make_async_copy(table.at[pl.ds(0, HOT), :], stage, ld_sem)
        big.start()
        big.wait()
        out = pltpu.make_async_copy(stage, buf.at[pl.ds(0, HOT), :], st_sem)
        out.start()
        out.wait()

    for k in range(CHUNKS):
        for dev in (1, 3, 5, 7):

            @pl.when(me == dev)
            def _(k=k):
                remote(table, a_rows(k), d_send.at[k], d_recv.at[k], 0).wait_recv()

        for dev in (2, 4, 6):

            @pl.when(me == dev)
            def _(k=k):
                remote(table, b_rows(k), d_send.at[k], d_recv.at[k], 0).wait_recv()

    for off in range(1, N_DEV):
        cold_in(off).wait_recv()
    for off in range(1, N_DEV):
        cold(off).wait_send()
    for k in range(CHUNKS):

        @pl.when(root)
        def _(k=k):
            remote(table, a_rows(k), a_send.at[k], a_recv.at[k], 2).wait_send()
            remote(table, b_rows(k), b_send.at[k], b_recv.at[k], 1).wait_send()
            remote(table, a_rows(k), d_send.at[k], d_recv.at[k], 1).wait_send()

        for dev in (2, 6, 4):

            @pl.when(me == dev)
            def _(k=k, dev=dev):
                if dev in nxt:
                    remote(buf, a_rows(k), a_send.at[k], a_recv.at[k], nxt[dev]).wait_send()
                remote(buf, a_rows(k), d_send.at[k], d_recv.at[k], dev + 1).wait_send()

        for dev in (1, 5, 7, 3):

            @pl.when(me == dev)
            def _(k=k, dev=dev):
                if dev in nxt:
                    remote(buf, b_rows(k), b_send.at[k], b_recv.at[k], nxt[dev]).wait_send()
                if dev != 1:
                    remote(buf, b_rows(k), d_send.at[k], d_recv.at[k], dev - 1).wait_send()


def lookup_exchange(table, send):
    dma = pltpu.SemaphoreType.DMA
    return pl.pallas_call(
        lookup_kernel,
        in_specs=[ANY] * 2,
        out_specs=ANY,
        out_shape=shape_of(BF16, BUF, D),
        scratch_shapes=[pltpu.VMEM((HOT, D), BF16), dma, dma] + [dma((CHUNKS,))] * 6 + [dma((N_DEV,))] * 2,
        compiler_params=params(collective_id=0, has_side_effects=True),
        cost_estimate=cost(8e10, 4e7),
        name="lookup_exchange",
    )(table, send)


def proj_kernel(x_ref, gain_ref, w_ref, bias_ref, cos_ref, sin_ref, hid_ref, qkv_ref):
    x = x_ref[...].astype(F32)
    inv = lax.rsqrt(row_mean(x * x) + NORM_EPS)
    hid = (x * inv * gain_ref[...]).astype(BF16)
    hid_ref[...] = hid
    cos_t = cos_ref[...]
    sin_t = sin_ref[...]
    for c in range(0, QKV, 512):
        lin = dot(hid, w_ref[:, c : c + 512], NN) + bias_ref[:, c : c + 512]
        for h in range(0, 512, HEAD_DIM):
            v = lin[:, h : h + HEAD_DIM]
            if c + h < D + KV * HEAD_DIM:
                v = v * cos_t + pltpu.roll(v, HEAD_DIM // 2, 1) * sin_t
            qkv_ref[:, c + h : c + h + HEAD_DIM] = v.astype(BF16)


def proj(x, gain, w, bias, cos_t, sin_t):
    tm = 256
    per = SEQ // tm
    return pl.pallas_call(
        proj_kernel,
        grid=(TOK // tm,),
        in_specs=[
            by_row(tm, D),
            full(1, D),
            full(D, QKV),
            full(1, QKV),
            pl.BlockSpec((tm, HEAD_DIM), lambda i: (lax.rem(i, per), 0)),
            pl.BlockSpec((tm, HEAD_DIM), lambda i: (lax.rem(i, per), 0)),
        ],
        out_specs=[by_row(tm, D), by_row(tm, QKV)],
        out_shape=[shape_of(BF16, TOK, D), shape_of(BF16, TOK, QKV)],
        compiler_params=params(),
        cost_estimate=cost(2 * TOK * D * QKV, 3e7),
        name="proj",
    )(x, gain, w, bias, cos_t, sin_t)


QB = 256
LOG2E = 1.4426950408889634


def rot_back(g, cos_t, sin_t):
    return g * cos_t - pltpu.roll(g, HEAD_DIM // 2, 1) * sin_t


def col_sums(g):
    return jnp.sum(g.reshape(g.shape[0] // 8, 8, g.shape[1]), axis=0)


def attn_kernel(q_ref, k_ref, v_ref, do_ref, cos_ref, sin_ref, o_ref, dq_ref, dk_ref, dv_ref, bq_ref, bk_ref, bv_ref, dk_acc, dv_acc):
    g = pl.program_id(2)
    scale = HEAD_DIM**-0.5

    @pl.when(g == 0)
    def _():
        dk_acc[...] = jnp.zeros_like(dk_acc)
        dv_acc[...] = jnp.zeros_like(dv_acc)

    bq = jnp.zeros((8, HEAD_DIM), F32)
    diag = lax.broadcasted_iota(I32, (QB, QB), 0) >= lax.broadcasted_iota(I32, (QB, QB), 1)
    for b in range(SEQ // QB):
        rows = slice(b * QB, (b + 1) * QB)
        n = (b + 1) * QB
        q = q_ref[rows, :]
        k = k_ref[:n, :]
        v = v_ref[:n, :]
        do = do_ref[rows, :]
        t = dot(q, k, NT) * (scale * LOG2E)
        last = jnp.where(diag, t[:, n - QB :], MASK_VALUE)
        t = last if b == 0 else jnp.concatenate([t[:, : n - QB], last], axis=1)
        e = jnp.exp2(t - jnp.max(t, axis=-1, keepdims=True))
        p = e * (1.0 / row_sum(e))
        pb = p.astype(BF16)
        o_ref[rows, :] = dot(pb, v, NN).astype(BF16)
        dp = dot(do, v, NT)
        delta = row_sum(dp * p)
        ds = (p * ((dp - delta) * scale)).astype(BF16)
        dq = rot_back(dot(ds, k, NN), cos_ref[rows, :], sin_ref[rows, :])
        bq = bq + col_sums(dq)
        dq_ref[rows, :] = dq.astype(BF16)
        dk_acc[:n, :] += dot(ds, q, TN)
        dv_acc[:n, :] += dot(pb, do, TN)
    bq_ref[0] = bq

    @pl.when(g == GROUP - 1)
    def _():
        dk = rot_back(dk_acc[...], cos_ref[...], sin_ref[...])
        dv = dv_acc[...]
        dk_ref[...] = dk.astype(BF16)
        dv_ref[...] = dv.astype(BF16)
        bk_ref[0] = col_sums(dk)
        bv_ref[0] = col_sums(dv)


def attention(qkv, d_attn, cos_t, sin_t):
    head = lambda b, h, g: (b, h * GROUP + g)
    kv = lambda b, h, g: (b, h)
    full = lambda b, h, g: (0, 0)
    blk = (SEQ, HEAD_DIM)
    return pl.pallas_call(
        attn_kernel,
        grid=(SEQS, KV, GROUP),
        in_specs=[
            pl.BlockSpec(blk, head),
            pl.BlockSpec(blk, lambda b, h, g: (b, HEADS + h)),
            pl.BlockSpec(blk, lambda b, h, g: (b, HEADS + KV + h)),
            pl.BlockSpec(blk, head),
            pl.BlockSpec(blk, full),
            pl.BlockSpec(blk, full),
        ],
        out_specs=[
            pl.BlockSpec(blk, head),
            pl.BlockSpec(blk, head),
            pl.BlockSpec(blk, kv),
            pl.BlockSpec(blk, kv),
            pl.BlockSpec((1, 8, HEAD_DIM), lambda b, h, g: (b, 0, h * GROUP + g)),
            pl.BlockSpec((1, 8, HEAD_DIM), lambda b, h, g: (b, 0, h)),
            pl.BlockSpec((1, 8, HEAD_DIM), lambda b, h, g: (b, 0, h)),
        ],
        out_shape=[
            shape_of(BF16, TOK, D),
            shape_of(BF16, TOK, D),
            shape_of(BF16, TOK, KV * HEAD_DIM),
            shape_of(BF16, TOK, KV * HEAD_DIM),
            shape_of(F32, SEQS, 8, D),
            shape_of(F32, SEQS, 8, KV * HEAD_DIM),
            shape_of(F32, SEQS, 8, KV * HEAD_DIM),
        ],
        scratch_shapes=[pltpu.VMEM((SEQ, HEAD_DIM), F32)] * 2,
        compiler_params=params(),
        cost_estimate=cost(6 * 2 * TOK * SEQ * D, 3e7),
        name="attention",
    )(qkv, qkv, qkv, d_attn, cos_t, sin_t)


def dx_kernel(dq_ref, dk_ref, dv_ref, w_ref, x_ref, go_ref, gain_ref, dx_ref, gg_ref, gg_acc):
    i = pl.program_id(0)

    @pl.when(i == 0)
    def _():
        gg_acc[...] = jnp.zeros_like(gg_acc)

    kvw = KV * HEAD_DIM
    dh = dot(dq_ref[...], w_ref[:, :D], NT)
    dh = dh + dot(dk_ref[...], w_ref[:, D : D + kvw], NT)
    dh = dh + dot(dv_ref[...], w_ref[:, D + kvw :], NT)
    x = x_ref[...].astype(F32)
    inv = lax.rsqrt(row_mean(x * x) + NORM_EPS)
    xn = x * inv
    gg_acc[...] += col_sums(dh * xn)
    dn = dh * gain_ref[...]
    mean = row_mean(dn * xn)
    dx_ref[...] = go_ref[...].astype(F32) + inv * (dn - xn * mean)
    gg_ref[...] = gg_acc[...]


def input_grad(dq, dk, dv, w, x, go, gain):
    tm = 256
    tok = lambda n: by_row(tm, n)
    return pl.pallas_call(
        dx_kernel,
        grid=(TOK // tm,),
        in_specs=[
            tok(D),
            tok(KV * HEAD_DIM),
            tok(KV * HEAD_DIM),
            full(D, QKV),
            tok(D),
            tok(D),
            full(1, D),
        ],
        out_specs=[tok(D), full(8, D)],
        out_shape=[shape_of(F32, TOK, D), shape_of(F32, 8, D)],
        scratch_shapes=[pltpu.VMEM((8, D), F32)],
        compiler_params=params(),
        cost_estimate=cost(2 * TOK * D * QKV, 4e7),
        name="input_grad",
    )(dq, dk, dv, w, x, go, gain)


def wgrad_kernel(h_ref, dq_ref, dk_ref, dv_ref, o_ref):
    h = h_ref[...]
    kvw = KV * HEAD_DIM
    o_ref[:, :D] = dot(h, dq_ref[...], TN)
    o_ref[:, D : D + kvw] = dot(h, dk_ref[...], TN)
    o_ref[:, D + kvw :] = dot(h, dv_ref[...], TN)


def qkv_weight_grad(hid, dq, dk, dv):
    tn = 256
    const = lambda n: full(TOK, n)
    return pl.pallas_call(
        wgrad_kernel,
        grid=(D // tn,),
        in_specs=[pl.BlockSpec((TOK, tn), lambda i: (0, i)), const(D), const(KV * HEAD_DIM), const(KV * HEAD_DIM)],
        out_specs=by_row(tn, QKV),
        out_shape=shape_of(F32, D, QKV),
        compiler_params=params(),
        cost_estimate=cost(2 * TOK * D * QKV, 3e7),
        name="qkv_weight_grad",
    )(hid, dq, dk, dv)


def scatter_kernel(xi_s, dx_ref, hot_ref, cold_ref, acc, sem):
    i = pl.program_id(0)
    tm = dx_ref.shape[0]

    @pl.when(i == 0)
    def _():
        def zero(b, c):
            acc[pl.ds(pl.multiple_of(b * LANE, LANE), LANE), :] = jnp.zeros((LANE, D), F32)
            return c

        lax.fori_loop(0, BUF // LANE, zero, 0)

    def body(q, c):
        for u in range(8):
            t = q * 8 + u
            r = xi_s[i * (tm // LANE) + lax.shift_right_logical(t, 7), jnp.bitwise_and(t, 127)]
            acc[pl.ds(r, 1), :] += dx_ref[pl.ds(t, 1), :]
        return c

    lax.fori_loop(0, tm // 8, body, 0)

    @pl.when(i == pl.num_programs(0) - 1)
    def _():
        a = pltpu.make_async_copy(acc.at[pl.ds(0, HOT), :], hot_ref, sem.at[0])
        b = pltpu.make_async_copy(acc.at[pl.ds(HOT, COLD), :], cold_ref, sem.at[1])
        a.start()
        b.start()
        a.wait()
        b.wait()


def scatter_rows(xi, dx):
    tm = 256
    return pl.pallas_call(
        scatter_kernel,
        grid_spec=pltpu.PrefetchScalarGridSpec(
            num_scalar_prefetch=1,
            grid=(TOK // tm,),
            in_specs=[by_row(tm, D)],
            out_specs=[ANY] * 2,
            scratch_shapes=[pltpu.VMEM((BUF, D), F32), pltpu.SemaphoreType.DMA((2,))],
        ),
        out_shape=[shape_of(F32, HOT, D), shape_of(F32, COLD, D)],
        compiler_params=params(),
        cost_estimate=cost(3e10, 5e7),
        name="scatter_rows",
    )(xi, dx)


ZROWS = 512


def final_kernel(me_s, own_s, tgt_s, rep_s, hot_ref, cold_ref, out_ref, zero, cold, acc, stage, hot, z_sem, c_sem, h_sem, p_sem):
    me = me_s[0]
    pltpu.make_async_copy(cold_ref, cold, c_sem).start()
    zero[...] = jnp.zeros_like(zero)

    def fill(lo, n):
        return pltpu.make_async_copy(zero.at[pl.ds(0, n), :], out_ref.at[pl.ds(lo, n), :], z_sem)

    spans = []
    lo = HOT
    while lo < ROWS:
        n = min(ZROWS, ROWS - lo)
        spans.append((lo, n))
        lo += n
    for lo, n in spans:
        fill(lo, n).start()

    @pl.when(me == 0)
    def _():
        pltpu.make_async_copy(hot_ref, hot, h_sem).start()

    @pl.when(me != 0)
    def _():
        for lo in range(0, HOT, ZROWS):
            fill(lo, ZROWS).start()

    def clear(b, c):
        acc[pl.ds(pl.multiple_of(b * LANE, LANE), LANE), :] = jnp.zeros((LANE, D), F32)
        return c

    lax.fori_loop(0, 2 * COLD // LANE, clear, 0)

    @pl.when(me == 0)
    def _():
        pltpu.make_async_copy(hot_ref, hot, h_sem).wait()
        pltpu.make_async_copy(hot, out_ref.at[pl.ds(0, HOT), :], h_sem).start()

    pltpu.make_async_copy(cold_ref, cold, c_sem).wait()

    def add(q, c):
        for u in range(8):
            j = q * 8 + u
            r = tgt_s[lax.shift_right_logical(j, 7), jnp.bitwise_and(j, 127)]
            acc[pl.ds(r, 1), :] += cold[pl.ds(j, 1), :]
        return c

    lax.fori_loop(0, COLD // 8, add, 0)

    def conv(b, c):
        rows = pl.ds(pl.multiple_of(b * LANE, LANE), LANE)
        stage[rows, :] = acc[rows, :].astype(BF16)
        return c

    lax.fori_loop(0, 2 * COLD // LANE, conv, 0)

    for lo, n in spans:
        fill(lo, n).wait()

    @pl.when(me == 0)
    def _():
        pltpu.make_async_copy(hot, out_ref.at[pl.ds(0, HOT), :], h_sem).wait()

    @pl.when(me != 0)
    def _():
        for lo in range(0, HOT, ZROWS):
            fill(lo, ZROWS).wait()

    def pair_copy(j, row):
        return pltpu.make_async_copy(
            stage.at[pl.ds(pl.multiple_of(j * 2, 2), 2), :], out_ref.at[pl.ds(pl.multiple_of(row, 2), 2), :], p_sem
        )

    def put(j, count):
        rep = rep_s[lax.shift_right_logical(j, 7), jnp.bitwise_and(j, 127)]
        s = lax.div(j, CAP)
        row = own_s[s, j - s * CAP]
        go = jnp.logical_and(rep == j, row >= 0)

        @pl.when(go)
        def _():
            pair_copy(j, lax.shift_right_logical(jnp.maximum(row, 0), 1) * 2).start()

        return count + go.astype(I32)

    count = lax.fori_loop(0, COLD, put, jnp.int32(0))

    def drain(j, c):
        pair_copy(0, 0).wait()
        return c

    lax.fori_loop(0, count, drain, 0)


def final_rows(me, own, tgt, rep, hot, cold):
    dma = pltpu.SemaphoreType.DMA
    return pl.pallas_call(
        final_kernel,
        grid_spec=pltpu.PrefetchScalarGridSpec(
            num_scalar_prefetch=4,
            grid=(1,),
            in_specs=[ANY] * 2,
            out_specs=ANY,
            scratch_shapes=[
                pltpu.VMEM((ZROWS, D), BF16),
                pltpu.VMEM((COLD, D), F32),
                pltpu.VMEM((2 * COLD, D), F32),
                pltpu.VMEM((2 * COLD, D), BF16),
                pltpu.VMEM((HOT, D), BF16),
                dma,
                dma,
                dma,
                dma,
            ],
        ),
        out_shape=shape_of(BF16, ROWS, D),
        compiler_params=params(),
        cost_estimate=cost(4e10, 8e7),
        name="final_rows",
    )(me, own, tgt, rep, hot, cold)


def swap_kernel(same, x_ref, out_ref, own_sem, send_sem, recv_sem):
    me = lax.axis_index("fsdp")
    barrier = pltpu.get_barrier_semaphore()
    for off in range(1, N_DEV):
        pl.semaphore_signal(barrier, inc=1, device_id=(lax.rem(me + off, N_DEV),), device_id_type=MESH)
    pl.semaphore_wait(barrier, N_DEV - 1)

    def copy(off):
        dst = lax.rem(me + off, N_DEV)
        return pltpu.make_async_remote_copy(
            src_ref=x_ref.at[0 if same else dst],
            dst_ref=out_ref.at[me],
            send_sem=send_sem.at[off],
            recv_sem=recv_sem.at[off],
            device_id=(dst,),
            device_id_type=MESH,
        )

    def inward(off):
        src = lax.rem(me - off + N_DEV, N_DEV)
        return pltpu.make_async_remote_copy(
            src_ref=x_ref.at[0],
            dst_ref=out_ref.at[src],
            send_sem=send_sem.at[off],
            recv_sem=recv_sem.at[off],
            device_id=(src,),
            device_id_type=MESH,
        )

    for off in range(1, N_DEV):
        copy(off).start()
    own = pltpu.make_async_copy(x_ref.at[0 if same else me], out_ref.at[me], own_sem)
    own.start()
    own.wait()
    for off in range(1, N_DEV):
        inward(off).wait_recv()
    for off in range(1, N_DEV):
        copy(off).wait_send()


def swap_blocks(x, cid):
    dma = pltpu.SemaphoreType.DMA
    return pl.pallas_call(
        functools.partial(swap_kernel, x.shape[0] == 1),
        in_specs=[ANY],
        out_specs=ANY,
        out_shape=jax.ShapeDtypeStruct((N_DEV,) + x.shape[1:], x.dtype),
        scratch_shapes=[dma, dma((N_DEV,)), dma((N_DEV,))],
        compiler_params=params(collective_id=cid, has_side_effects=True),
        name="swap_blocks",
    )(x)


SLOW = LANE


def general_lookup(table, ids, first):
    def step(c, x):
        loc = lax.dynamic_slice(ids, (0, c * SLOW), (N_DEV, SLOW)) - first
        owned = (loc >= 0) & (loc < ROWS)
        rows = jnp.take(table, jnp.where(owned, loc, 0), axis=0)
        rows = jnp.where(owned[..., None], rows, jnp.zeros((), BF16))
        got = swap_blocks(rows, 1).astype(F32).sum(0).astype(BF16)
        return lax.dynamic_update_slice(x, got, (c * SLOW, 0))

    return lax.fori_loop(0, TOK // SLOW, step, jnp.zeros((TOK, D), BF16))


def general_scatter(d_x, ids, first):
    def step(c, acc):
        loc = lax.dynamic_slice(ids, (0, c * SLOW), (N_DEV, SLOW)) - first
        owned = (loc >= 0) & (loc < ROWS)
        got = swap_blocks(lax.dynamic_slice(d_x, (c * SLOW, 0), (SLOW, D))[None], 2)
        seg = jnp.where(owned, loc, ROWS)
        return acc.at[seg.reshape(-1)].add(got.reshape(-1, D), mode="drop")

    acc = lax.fori_loop(0, TOK // SLOW, step, jnp.zeros((ROWS, D), F32))
    return acc.astype(BF16)


def rope_tables():
    half = HEAD_DIM // 2
    inv_freq = jnp.power(ROPE_THETA, -(jnp.arange(half, dtype=F32) * 2.0 / HEAD_DIM))
    angles = jnp.arange(SEQ, dtype=F32)[:, None] * inv_freq[None, :]
    cos_h, sin_h = jnp.cos(angles), jnp.sin(angles)
    return jnp.concatenate([cos_h, cos_h], axis=-1), jnp.concatenate([-sin_h, sin_h], axis=-1)


def device_step(tok_ids, grad_out, table, gain_p, wq_p, bq_p, wk_p, bk_p, wv_p, bv_p, wo_p):
    ax = "fsdp"
    me = lax.axis_index(ax)
    me1 = me.reshape(1).astype(I32)
    first = me * ROWS
    kvw = KV * HEAD_DIM
    mine = tok_ids.reshape(1, TOK).astype(F32)
    small = jnp.concatenate([mine[0]] + [v.astype(F32) for v in (gain_p, bq_p, bk_p, bv_p)])
    small = lax.all_gather(small, ax)
    w_qkv = lax.all_gather(jnp.concatenate([wq_p, wk_p, wv_p], axis=1), ax, axis=0, tiled=True)
    w_out = lax.all_gather(wo_p, ax, axis=0, tiled=True)
    ids_f = small[:, :TOK]
    cuts = [TOK, TOK + D // N_DEV, TOK + 2 * (D // N_DEV), TOK + 2 * (D // N_DEV) + kvw // N_DEV, TOK + 2 * (D // N_DEV) + 2 * (kvw // N_DEV)]
    gain, b_q, b_k, b_v = (small[:, a:b].reshape(1, -1) for a, b in zip(cuts[:-1], cuts[1:], strict=True))
    bias = jnp.concatenate([b_q, b_k, b_v], axis=1)
    cos_t, sin_t = rope_tables()

    xi, own, most = index_maps(me1, mine, jnp.repeat(ids_f.T, N_DEV, axis=1))
    over = most[0, 0] > CAP
    send = gather_rows(table, own, CAP)
    buf = lookup_exchange(table, send)
    x = lax.cond(
        over,
        lambda: general_lookup(table, ids_f.astype(I32), first).reshape(TOK, D),
        lambda: gather_rows(buf, xi, LANE).reshape(TOK, D),
    )
    x = lax.optimization_barrier(x)
    go = grad_out.reshape(TOK, D)

    hid, qkv = proj(x, gain, w_qkv, bias, cos_t, sin_t)
    d_attn = dot(go, w_out, NT).astype(BF16)
    attn, dq, dk, dv, s_q, s_k, s_v = attention(qkv, d_attn, cos_t, sin_t)
    block_out = (x.astype(F32) + dot(attn, w_out, NN)).astype(BF16).reshape(grad_out.shape)
    g_out = lax.psum_scatter(dot(attn, go, TN), ax, scatter_dimension=0, tiled=True)
    d_x, s_g = input_grad(dq, dk, dv, w_qkv, x, go, gain)
    g_qkv = lax.psum_scatter(qkv_weight_grad(hid, dq, dk, dv), ax, scatter_dimension=0, tiled=True)

    parts = [s_g.sum(0), s_q.sum((0, 1)), s_k.sum((0, 1)), s_v.sum((0, 1))]
    vec = jnp.concatenate([p.reshape(N_DEV, -1) for p in parts], axis=1)
    vec = lax.all_to_all(vec, ax, 0, 0, tiled=True).sum(0)

    hot, cold = scatter_rows(xi, d_x)
    cold = lax.all_to_all(cold.reshape(N_DEV, CAP, D), ax, 0, 0, tiled=True).reshape(COLD, D)
    hot = lax.psum_scatter(hot, ax, scatter_dimension=0, tiled=True).astype(BF16)
    hot = lax.all_gather(hot, ax, axis=0, tiled=True)
    flat = own[:, :CAP].reshape(1, COLD).astype(F32)
    tgt, rep = merge_maps(flat, flat.reshape(COLD, 1))
    grad_table = lax.cond(
        over,
        lambda: general_scatter(d_x, ids_f.astype(I32), first),
        lambda: final_rows(me1, own, tgt, rep, hot, cold),
    )

    e0, e1, e2 = D // N_DEV, 2 * (D // N_DEV), 2 * (D // N_DEV) + kvw // N_DEV
    return (
        block_out,
        grad_table,
        vec[:e0],
        g_qkv[:, :D],
        vec[e0:e1],
        g_qkv[:, D : D + kvw],
        vec[e1:e2],
        g_qkv[:, D + kvw :],
        vec[e2:],
        g_out,
    )


def solution(mesh):
    row = P("fsdp", None)
    vec = P("fsdp")
    act = P("fsdp", None, None)
    weights = (vec, row, vec, row, vec, row, vec, row)
    return jax.shard_map(
        device_step, mesh=mesh, in_specs=(row, act, row) + weights, out_specs=(act, row) + weights, check_vma=False
    )
```

```python
import functools

import jax
import jax.numpy as jnp
from jax import lax
from jax.experimental import pallas as pl
from jax.experimental.pallas import tpu as pltpu
from jax.sharding import PartitionSpec as P

F32 = jnp.float32
BF16 = jnp.bfloat16
I32 = jnp.int32
MESH = pl.DeviceIdType.MESH

LANE = 128
SUB = 8
HEAD_DIM = LANE
ROPE_THETA = 1.0e6
NORM_EPS = 1e-6
MASK_VALUE = -1e30

N_DEV = 8
OTHERS = range(1, N_DEV)
SEQ = 1024
SEQS = 2
TOK = SEQ * SEQS
D = 1536
HEADS = 12
KV = 2
GROUP = HEADS // KV
ROWS = 18992
HOT = 4096
CAP = 176
COLD = N_DEV * CAP
BUF = HOT + COLD
QKV = D + 2 * KV * HEAD_DIM
VMEM_MAX = 66_000_000


def params(**kw):
    return pltpu.CompilerParams(vmem_limit_bytes=VMEM_MAX, **kw)


ANY = pl.BlockSpec(memory_space=pl.ANY)


def full(*shape):
    return pl.BlockSpec(shape, lambda *i: (0,) * len(shape))


def by_row(*shape):
    return pl.BlockSpec(shape, lambda i, *_: (i,) + (0,) * (len(shape) - 1))


def shape_of(dtype, *shape):
    return jax.ShapeDtypeStruct(shape, dtype)


def row_sum(v):
    return jnp.sum(v, axis=-1, keepdims=True)


def row_mean(v):
    return jnp.mean(v, axis=-1, keepdims=True)


def col_sum(v):
    return jnp.sum(v, axis=0, keepdims=True)


def loop(n, body):
    def step(k, c):
        body(k)
        return c

    lax.fori_loop(0, n, step, 0)


def iota(dtype, shape, dim):
    return lax.broadcasted_iota(I32, shape, dim).astype(dtype)


def cost(flops, nbytes):
    return pl.CostEstimate(flops=int(flops), bytes_accessed=int(nbytes), transcendentals=0)


def dot(a, b, dims):
    return lax.dot_general(a, b, (dims, ((), ())), preferred_element_type=F32)


NN = ((1,), (0,))
NT = ((1,), (1,))
TN = ((0,), (0,))


HALF = HOT // 2
CHUNKS = 16
PACK = 20


def meet(me):
    barrier = pltpu.get_barrier_semaphore()
    for off in OTHERS:
        pl.semaphore_signal(barrier, inc=1, device_id=(lax.rem(me + off, N_DEV),), device_id_type=MESH)
    pl.semaphore_wait(barrier, N_DEV - 1)


def push(src, dst, s_sem, r_sem, dev):
    return pltpu.make_async_remote_copy(
        src_ref=src, dst_ref=dst, send_sem=s_sem, recv_sem=r_sem, device_id=(dev,), device_id_type=MESH
    )


def rows_of(ref, start, n, align=SUB):
    return ref.at[pl.ds(pl.multiple_of(start, align), n), :]


def prologue_kernel(pk_ref, table, hot, all_ref, xi_ref, hid_ref, cold_ref, own_ref, most_ref, got, code, own_f, stage, ld_sem, p_send, p_recv, c_send, c_recv, d_send, d_recv):
    me = lax.axis_index("fsdp")
    n = HALF // CHUNKS
    got[me] = pk_ref[...]
    meet(me)

    def pack_to(off):
        return push(pk_ref, got.at[me], p_send.at[off], p_recv.at[off], lax.rem(me + off, N_DEV))

    def pack_from(off):
        src = lax.rem(me - off + N_DEV, N_DEV)
        return push(pk_ref, got.at[src], p_send.at[off], p_recv.at[off], src)

    for off in OTHERS:
        pack_to(off).start()

    def part(ref, half, k):
        return rows_of(ref, half * HALF + k * n, n)

    def chain(src, half, k, dev):
        return push(part(src, half, k), part(hot, half, k), c_send.at[k], c_recv.at[k], dev)

    def pass_on(src, half, k, dev):
        return push(part(src, half, k), part(hot, half, k), d_send.at[k], d_recv.at[k], dev)

    def root_copy():
        return pltpu.make_async_copy(rows_of(table, 0, HOT), stage, ld_sem)

    def root_store():
        return pltpu.make_async_copy(stage, hot, ld_sem)

    nxt = {2: 6, 6: 4, 1: 5, 5: 7, 7: 3}

    @pl.when(me == 0)
    def _():
        def go(k):
            chain(table, 0, k, 2).start()
            pass_on(table, 1, k, 1).start()

        loop(CHUNKS, go)
        root_copy().start()

    r_io = iota(I32, (LANE, LANE), 0)
    c_io = iota(I32, (LANE, LANE), 1)
    own_s = iota(I32, (N_DEV, 1), 0)
    lo_s = jnp.maximum(own_s * ROWS, HOT).astype(F32)
    hi_s = (own_s * ROWS + ROWS).astype(F32)
    up = (r_io < c_io).astype(BF16)
    run = jnp.zeros((N_DEV, 1), F32)
    for b in range(TOK // LANE):
        blk = pk_ref[b : b + 1, :]
        hit = jnp.logical_and(blk >= lo_s, blk < hi_s)
        one = hit.astype(F32)
        rank = dot(one.astype(BF16), up, NN) + run
        run = run + row_sum(one)
        slot = jnp.minimum(rank, CAP - 1) + own_s.astype(F32) * CAP
        slot = col_sum(jnp.where(hit, slot, 0.0))
        is_hot = blk < HOT
        xi_ref[b : b + 1, :] = jnp.where(is_hot, blk, slot + HOT).astype(I32)
        hid_ref[b : b + 1, :] = jnp.where(is_hot, blk, -1.0).astype(I32)
        cold_ref[b : b + 1, :] = jnp.where(is_hot, -1.0, slot).astype(I32)

    for off in OTHERS:
        pack_from(off).wait_recv()
    all_ref[...] = got[...]
    per = TOK // LANE
    grid = jnp.concatenate([got[s][:per, :] for s in range(N_DEV)], axis=0)
    same = (lax.div(r_io[: N_DEV * per, : N_DEV * per], per) == lax.div(c_io[: N_DEV * per, : N_DEV * per], per)).astype(F32)
    tot = jnp.zeros((1, N_DEV * per), F32)
    flat = grid.T
    for o in range(N_DEV):
        hit = jnp.logical_and(flat >= max(o * ROWS, HOT), flat < (o + 1) * ROWS)
        cnt = jnp.broadcast_to(col_sum(hit.astype(F32)), (SUB, N_DEV * per))
        tot = jnp.maximum(tot, dot(cnt.astype(BF16), same.astype(BF16), NN)[:1, :])
    most_ref[...] = jnp.broadcast_to(jnp.max(tot, axis=-1, keepdims=True), most_ref.shape)
    first = (me * ROWS).astype(F32)
    hit = jnp.logical_and(flat >= jnp.maximum(me * ROWS, HOT).astype(F32), flat < first + ROWS)
    one = hit.astype(F32)
    rank = dot((r_io > c_io).astype(BF16), one.astype(BF16), NN)
    before = jnp.where(r_io < c_io, 1.0, 0.0)[: N_DEV * per, : N_DEV * per] * same
    cnt = jnp.broadcast_to(col_sum(one), (SUB, N_DEV * per))
    rank = rank + dot(cnt.astype(BF16), before.astype(BF16), NN)[:1, :]
    code[...] = jnp.where(hit, rank * CODE + (flat - first), -1.0)
    own_f[...] = jnp.zeros_like(own_f)
    slots = iota(F32, (1, 2 * LANE), 1)
    lane = iota(I32, (1, N_DEV * per), 1)

    def listing(c):
        val = row_sum(jnp.where(lane == c, code[...], 0.0))
        rk = jnp.floor(val * (1.0 / CODE))
        loc = val - rk * CODE + 1.0
        add = col_sum(jnp.where(rk == slots, loc, 0.0))
        s = lax.div(c, per)
        own_f[pl.ds(s, 1), :] += add

    def chunk(k):
        @pl.when(me == 0)
        def _():
            chain(table, 0, k, 2).wait_send()
            chain(table, 0, k, 1).start()

        for dev in (2, 6, 4, 1, 5, 7, 3):
            half = dev % 2

            @pl.when(me == dev)
            def _(dev=dev, half=half):
                if dev == 1:
                    pass_on(table, half, k, 0).wait_recv()
                else:
                    chain(table, half, k, 0).wait_recv()
                if dev in nxt:
                    chain(hot, half, k, nxt[dev]).start()
                if dev != 1:
                    pass_on(hot, half, k, dev + 1 - 2 * half).start()

        for u in range(N_DEV * per // CHUNKS):
            listing(k * (N_DEV * per // CHUNKS) + u)

    loop(CHUNKS, chunk)
    own_ref[...] = own_f[...].astype(I32) - 1

    @pl.when(me == 0)
    def _():
        root_copy().wait()
        root_store().start()

    def tail(k):
        @pl.when(me == 0)
        def _():
            chain(table, 0, k, 1).wait_send()
            pass_on(table, 1, k, 1).wait_send()

        @pl.when(me == 1)
        def _():
            chain(table, 0, k, 0).wait_recv()
            chain(hot, 1, k, 5).wait_send()

        for dev in (2, 6, 4, 5, 7, 3):
            half = dev % 2

            @pl.when(me == dev)
            def _(dev=dev, half=half):
                pass_on(table, 1 - half, k, 0).wait_recv()
                if dev in nxt:
                    chain(hot, half, k, nxt[dev]).wait_send()
                pass_on(hot, half, k, dev + 1 - 2 * half).wait_send()

    loop(CHUNKS, tail)
    for off in OTHERS:
        pack_to(off).wait_send()

    @pl.when(me == 0)
    def _():
        root_store().wait()


CODE = 32768.0


def prologue(pk, table):
    dma = pltpu.SemaphoreType.DMA
    per = TOK // LANE
    vm = pl.BlockSpec(memory_space=pltpu.VMEM)
    return pl.pallas_call(
        prologue_kernel,
        in_specs=[vm, ANY],
        out_specs=[ANY] + [vm] * 6,
        out_shape=[
            shape_of(BF16, HOT, D),
            shape_of(F32, N_DEV, PACK, LANE),
            shape_of(I32, per, LANE),
            shape_of(I32, per, LANE),
            shape_of(I32, per, LANE),
            shape_of(I32, N_DEV, 2 * LANE),
            shape_of(F32, SUB, LANE),
        ],
        scratch_shapes=[
            pltpu.VMEM((N_DEV, PACK, LANE), F32),
            pltpu.VMEM((LANE, N_DEV * per), F32),
            pltpu.VMEM((N_DEV, 2 * LANE), F32),
            pltpu.VMEM((HOT, D), BF16),
            dma,
            dma((N_DEV,)),
            dma((N_DEV,)),
        ]
        + [dma((CHUNKS,))] * 4,
        compiler_params=params(collective_id=0, has_side_effects=True),
        cost_estimate=cost(8e10, 4e7),
        name="prologue",
    )(pk, table)


def merge_kernel(row_ref, col_ref, tgt_ref, rep_ref):
    n = row_ref.shape[1]
    for b in range(n // LANE):
        row = row_ref[:, b * LANE : (b + 1) * LANE]
        pair = jnp.floor(row * 0.5)
        best = jnp.full((8, LANE), float(n), F32)
        for c in range(n // LANE):
            other = jnp.floor(col_ref[c * LANE : (c + 1) * LANE, :] * 0.5)
            kk = (lax.broadcasted_iota(I32, (LANE, 1), 0) + c * LANE).astype(F32)
            hit = jnp.where(other == pair, kk, float(n))
            best = jnp.minimum(best, jnp.min(hit.reshape(16, 8, LANE), axis=0))
        rep = jnp.min(best, axis=0, keepdims=True)
        par = row - 2.0 * pair
        tgt_ref[b : b + 1, :] = (2.0 * rep + par).astype(I32)
        rep_ref[b : b + 1, :] = rep.astype(I32)


def merge_maps(row, col):
    n = row.shape[1]
    return pl.pallas_call(
        merge_kernel,
        out_shape=[shape_of(I32, n // LANE, LANE)] * 2,
        compiler_params=params(),
        cost_estimate=cost(5e9, 1e6),
        name="merge_maps",
    )(row, col)


def gather_kernel(n, idx_s, idx_ref, src_ref, out_ref, buf, sem):
    i = pl.program_id(0)

    def fetch(blk, slot):
        def body(q):
            for u in range(8):
                j = q * 8 + u
                r = lax.shift_right_logical(jnp.maximum(idx_s[blk, j], 0), 1)
                pltpu.make_async_copy(
                    src_ref.at[pl.ds(pl.multiple_of(r * 2, 2), 2), :],
                    buf.at[slot, pl.ds(pl.multiple_of(j * 2, 2), 2), :],
                    sem.at[slot],
                ).start()

        loop(n // 8, body)

    slot = lax.rem(i, 2)

    @pl.when(i == 0)
    def _():
        fetch(0, 0)

    @pl.when(i + 1 < pl.num_programs(0))
    def _():
        fetch(i + 1, 1 - slot)

    idx = idx_ref[pl.ds(i, 1), :][:, :n]
    k_io = lax.broadcasted_iota(I32, (2 * n, n), 0)
    j_io = lax.broadcasted_iota(I32, (2 * n, n), 1)
    want = jnp.where(idx < 0, -1, 2 * j_io + jnp.bitwise_and(idx, 1))
    pick = (k_io == want).astype(BF16)
    pltpu.make_async_copy(src_ref.at[pl.ds(0, 2 * n), :], buf.at[slot], sem.at[slot]).wait()
    out_ref[0] = dot(pick, buf[slot], TN).astype(BF16)


def gather_rows(src, idx, n):
    blocks = idx.shape[0]
    return pl.pallas_call(
        functools.partial(gather_kernel, n),
        grid_spec=pltpu.PrefetchScalarGridSpec(
            num_scalar_prefetch=1,
            grid=(blocks,),
            in_specs=[full(*idx.shape), ANY],
            out_specs=by_row(1, n, D),
            scratch_shapes=[pltpu.VMEM((2, 2 * n, D), BF16), pltpu.SemaphoreType.DMA((2,))],
        ),
        out_shape=shape_of(BF16, blocks, n, D),
        compiler_params=params(),
        cost_estimate=cost(2e10, blocks * n * D * 6),
        name="gather_rows",
    )(idx, idx, src)


def proj_kernel(xh_ref, slot_ref, cold_ref, gain_ref, w_ref, bias_ref, cos_ref, sin_ref, x_ref, hid_ref, qkv_ref):
    tm = xh_ref.shape[0]
    picked = []
    for b in range(tm // LANE):
        slot = slot_ref[pl.ds(pl.program_id(0) * (tm // LANE) + b, 1), :]
        pick = (iota(I32, (COLD, LANE), 0) == slot).astype(F32).astype(BF16)
        picked.append(dot(pick, cold_ref[...], TN))
    x = xh_ref[...].astype(F32) + jnp.concatenate(picked, axis=0)
    x_ref[...] = x.astype(BF16)
    inv = lax.rsqrt(row_mean(x * x) + NORM_EPS)
    hid = (x * inv * gain_ref[...]).astype(BF16)
    hid_ref[...] = hid
    cos_t = cos_ref[...]
    sin_t = sin_ref[...]
    wide = 4 * HEAD_DIM
    for c in range(0, QKV, wide):
        lin = dot(hid, w_ref[:, c : c + wide], NN) + bias_ref[:, c : c + wide]
        for h in range(0, wide, HEAD_DIM):
            v = lin[:, h : h + HEAD_DIM]
            if c + h < D + KV * HEAD_DIM:
                v = v * cos_t + pltpu.roll(v, HEAD_DIM // 2, 1) * sin_t
            qkv_ref[:, c + h : c + h + HEAD_DIM] = v.astype(BF16)


def proj(xh, slot, cold, gain, w, bias, cos_t, sin_t):
    tm = 2 * LANE
    per = SEQ // tm
    turn = pl.BlockSpec((tm, HEAD_DIM), lambda i: (lax.rem(i, per), 0))
    return pl.pallas_call(
        proj_kernel,
        grid=(TOK // tm,),
        in_specs=[by_row(tm, D), full(*slot.shape), full(COLD, D), full(1, D), full(D, QKV), full(1, QKV), turn, turn],
        out_specs=[by_row(tm, D), by_row(tm, D), by_row(tm, QKV)],
        out_shape=[shape_of(BF16, TOK, D), shape_of(BF16, TOK, D), shape_of(BF16, TOK, QKV)],
        compiler_params=params(),
        cost_estimate=cost(2 * TOK * D * (QKV + COLD), 3e7),
        name="proj",
    )(xh, slot, cold, gain, w, bias, cos_t, sin_t)


QB = 256
LOG2E = 1.4426950408889634


def rot_back(g, cos_t, sin_t):
    return g * cos_t - pltpu.roll(g, HEAD_DIM // 2, 1) * sin_t


def col_sums(g):
    return jnp.sum(g.reshape(g.shape[0] // 8, 8, g.shape[1]), axis=0)


def attn_kernel(q_ref, k_ref, v_ref, do_ref, cos_ref, sin_ref, o_ref, dq_ref, dk_ref, dv_ref, bq_ref, bk_ref, bv_ref, dk_acc, dv_acc):
    g = pl.program_id(2)
    scale = HEAD_DIM**-0.5

    @pl.when(g == 0)
    def _():
        dk_acc[...] = jnp.zeros_like(dk_acc)
        dv_acc[...] = jnp.zeros_like(dv_acc)

    bq = jnp.zeros((8, HEAD_DIM), F32)
    diag = lax.broadcasted_iota(I32, (QB, QB), 0) >= lax.broadcasted_iota(I32, (QB, QB), 1)
    for b in range(SEQ // QB):
        rows = slice(b * QB, (b + 1) * QB)
        n = (b + 1) * QB
        q = q_ref[rows, :]
        k = k_ref[:n, :]
        v = v_ref[:n, :]
        do = do_ref[rows, :]
        t = dot(q, k, NT) * (scale * LOG2E)
        last = jnp.where(diag, t[:, n - QB :], MASK_VALUE)
        t = last if b == 0 else jnp.concatenate([t[:, : n - QB], last], axis=1)
        e = jnp.exp2(t - jnp.max(t, axis=-1, keepdims=True))
        p = e * (1.0 / row_sum(e))
        pb = p.astype(BF16)
        o_ref[rows, :] = dot(pb, v, NN).astype(BF16)
        dp = dot(do, v, NT)
        delta = row_sum(dp * p)
        ds = (p * ((dp - delta) * scale)).astype(BF16)
        dq = rot_back(dot(ds, k, NN), cos_ref[rows, :], sin_ref[rows, :])
        bq = bq + col_sums(dq)
        dq_ref[rows, :] = dq.astype(BF16)
        dk_acc[:n, :] += dot(ds, q, TN)
        dv_acc[:n, :] += dot(pb, do, TN)
    bq_ref[0] = bq

    @pl.when(g == GROUP - 1)
    def _():
        dk = rot_back(dk_acc[...], cos_ref[...], sin_ref[...])
        dv = dv_acc[...]
        dk_ref[...] = dk.astype(BF16)
        dv_ref[...] = dv.astype(BF16)
        bk_ref[0] = col_sums(dk)
        bv_ref[0] = col_sums(dv)


def attention(qkv, d_attn, cos_t, sin_t):
    head = lambda b, h, g: (b, h * GROUP + g)
    kv = lambda b, h, g: (b, h)
    full = lambda b, h, g: (0, 0)
    blk = (SEQ, HEAD_DIM)
    return pl.pallas_call(
        attn_kernel,
        grid=(SEQS, KV, GROUP),
        in_specs=[
            pl.BlockSpec(blk, head),
            pl.BlockSpec(blk, lambda b, h, g: (b, HEADS + h)),
            pl.BlockSpec(blk, lambda b, h, g: (b, HEADS + KV + h)),
            pl.BlockSpec(blk, head),
            pl.BlockSpec(blk, full),
            pl.BlockSpec(blk, full),
        ],
        out_specs=[
            pl.BlockSpec(blk, head),
            pl.BlockSpec(blk, head),
            pl.BlockSpec(blk, kv),
            pl.BlockSpec(blk, kv),
            pl.BlockSpec((1, 8, HEAD_DIM), lambda b, h, g: (b, 0, h * GROUP + g)),
            pl.BlockSpec((1, 8, HEAD_DIM), lambda b, h, g: (b, 0, h)),
            pl.BlockSpec((1, 8, HEAD_DIM), lambda b, h, g: (b, 0, h)),
        ],
        out_shape=[
            shape_of(BF16, TOK, D),
            shape_of(BF16, TOK, D),
            shape_of(BF16, TOK, KV * HEAD_DIM),
            shape_of(BF16, TOK, KV * HEAD_DIM),
            shape_of(F32, SEQS, 8, D),
            shape_of(F32, SEQS, 8, KV * HEAD_DIM),
            shape_of(F32, SEQS, 8, KV * HEAD_DIM),
        ],
        scratch_shapes=[pltpu.VMEM((SEQ, HEAD_DIM), F32)] * 2,
        compiler_params=params(),
        cost_estimate=cost(6 * 2 * TOK * SEQ * D, 3e7),
        name="attention",
    )(qkv, qkv, qkv, d_attn, cos_t, sin_t)


def dx_kernel(dq_ref, dk_ref, dv_ref, w_ref, x_ref, go_ref, gain_ref, dx_ref, gg_ref, gg_acc):
    i = pl.program_id(0)

    @pl.when(i == 0)
    def _():
        gg_acc[...] = jnp.zeros_like(gg_acc)

    kvw = KV * HEAD_DIM
    dh = dot(dq_ref[...], w_ref[:, :D], NT)
    dh = dh + dot(dk_ref[...], w_ref[:, D : D + kvw], NT)
    dh = dh + dot(dv_ref[...], w_ref[:, D + kvw :], NT)
    x = x_ref[...].astype(F32)
    inv = lax.rsqrt(row_mean(x * x) + NORM_EPS)
    xn = x * inv
    gg_acc[...] += col_sums(dh * xn)
    dn = dh * gain_ref[...]
    mean = row_mean(dn * xn)
    dx_ref[...] = go_ref[...].astype(F32) + inv * (dn - xn * mean)
    gg_ref[...] = gg_acc[...]


def input_grad(dq, dk, dv, w, x, go, gain):
    tm = 256
    tok = lambda n: by_row(tm, n)
    return pl.pallas_call(
        dx_kernel,
        grid=(TOK // tm,),
        in_specs=[
            tok(D),
            tok(KV * HEAD_DIM),
            tok(KV * HEAD_DIM),
            full(D, QKV),
            tok(D),
            tok(D),
            full(1, D),
        ],
        out_specs=[tok(D), full(8, D)],
        out_shape=[shape_of(F32, TOK, D), shape_of(F32, 8, D)],
        scratch_shapes=[pltpu.VMEM((8, D), F32)],
        compiler_params=params(),
        cost_estimate=cost(2 * TOK * D * QKV, 4e7),
        name="input_grad",
    )(dq, dk, dv, w, x, go, gain)


def wgrad_kernel(h_ref, dq_ref, dk_ref, dv_ref, o_ref):
    h = h_ref[...]
    kvw = KV * HEAD_DIM
    o_ref[:, :D] = dot(h, dq_ref[...], TN)
    o_ref[:, D : D + kvw] = dot(h, dk_ref[...], TN)
    o_ref[:, D + kvw :] = dot(h, dv_ref[...], TN)


def qkv_weight_grad(hid, dq, dk, dv):
    tn = 256
    const = lambda n: full(TOK, n)
    return pl.pallas_call(
        wgrad_kernel,
        grid=(D // tn,),
        in_specs=[pl.BlockSpec((TOK, tn), lambda i: (0, i)), const(D), const(KV * HEAD_DIM), const(KV * HEAD_DIM)],
        out_specs=by_row(tn, QKV),
        out_shape=shape_of(F32, D, QKV),
        compiler_params=params(),
        cost_estimate=cost(2 * TOK * D * QKV, 3e7),
        name="qkv_weight_grad",
    )(hid, dq, dk, dv)


def scatter_kernel(xi_s, dx_ref, hot_ref, cold_ref, acc, sem):
    i = pl.program_id(0)
    tm = dx_ref.shape[0]

    @pl.when(i == 0)
    def _():
        def zero(b):
            acc[pl.ds(pl.multiple_of(b * LANE, LANE), LANE), :] = jnp.zeros((LANE, D), F32)

        loop(BUF // LANE, zero)

    def body(q):
        for u in range(8):
            t = q * 8 + u
            r = xi_s[i * (tm // LANE) + lax.shift_right_logical(t, 7), jnp.bitwise_and(t, 127)]
            acc[pl.ds(r, 1), :] += dx_ref[pl.ds(t, 1), :]

    loop(tm // 8, body)

    @pl.when(i == pl.num_programs(0) - 1)
    def _():
        a = pltpu.make_async_copy(acc.at[pl.ds(0, HOT), :], hot_ref, sem.at[0])
        b = pltpu.make_async_copy(acc.at[pl.ds(HOT, COLD), :], cold_ref, sem.at[1])
        a.start()
        b.start()
        a.wait()
        b.wait()


def scatter_rows(xi, dx):
    tm = 256
    return pl.pallas_call(
        scatter_kernel,
        grid_spec=pltpu.PrefetchScalarGridSpec(
            num_scalar_prefetch=1,
            grid=(TOK // tm,),
            in_specs=[by_row(tm, D)],
            out_specs=[ANY] * 2,
            scratch_shapes=[pltpu.VMEM((BUF, D), F32), pltpu.SemaphoreType.DMA((2,))],
        ),
        out_shape=[shape_of(F32, HOT, D), shape_of(F32, COLD, D)],
        compiler_params=params(),
        cost_estimate=cost(3e10, 5e7),
        name="scatter_rows",
    )(xi, dx)


PIECES = 32


def reduce_kernel(hot, cold, out_hot, out_cold, mine, pair, above, done, stage, l_sem, s_sem, x_send, x_recv, c_send, c_recv, h_send, h_recv, o_sem, o_recv):
    me = lax.axis_index("fsdp")
    half = mine.shape[0]
    n = half // PIECES
    core = lax.rem(me, 2)
    other = me + 1 - 2 * core
    meet(me)

    def part(ref, k):
        return rows_of(ref, k * n, n)

    def load(k):
        return pltpu.make_async_copy(rows_of(hot, core * half + k * n, n), part(mine, k), l_sem.at[k])

    def trade(k):
        return push(rows_of(hot, (1 - core) * half + k * n, n), part(pair, k), x_send.at[k], x_recv.at[k], other)

    def cold_to(off):
        dst = lax.rem(me + off, N_DEV)
        return push(cold.at[dst], out_cold.at[me], c_send.at[off], c_recv.at[off], dst)

    def cold_from(off):
        src = lax.rem(me - off + N_DEV, N_DEV)
        return push(cold.at[0], out_cold.at[src], c_send.at[off], c_recv.at[off], src)

    def hand(k, dev):
        return push(part(mine, k), part(above, k), h_send.at[k], h_recv.at[k], dev)

    def keep(k):
        return pltpu.make_async_copy(part(done, k), part(out_hot, k), o_sem.at[k])

    def give(k):
        return push(part(done, k), rows_of(out_hot, half + k * n, n), o_sem.at[k], o_recv.at[k], 0)

    def begin(k):
        load(k).start()
        trade(k).start()

    loop(PIECES, begin)
    for off in OTHERS:
        cold_to(off).start()
    own_in = pltpu.make_async_copy(cold.at[me], stage, s_sem)
    own_in.start()
    own_in.wait()
    own_out = pltpu.make_async_copy(stage, out_cold.at[me], s_sem)
    own_out.start()
    nxt = {4: 6, 6: 2, 2: 0, 3: 7, 7: 5, 5: 1}
    head = jnp.logical_or(me == 4, me == 3)
    end = me < 2

    def step(k):
        rows = pl.ds(pl.multiple_of(k * n, SUB), n)
        load(k).wait()
        trade(k).wait_recv()

        @pl.when(head)
        def _():
            mine[rows, :] = mine[rows, :] + pair[rows, :]

        @pl.when(jnp.logical_not(head))
        def _():
            hand(k, 0).wait_recv()
            mine[rows, :] = mine[rows, :] + pair[rows, :] + above[rows, :]

        for dev, to in nxt.items():

            @pl.when(me == dev)
            def _(to=to):
                hand(k, to).start()

        @pl.when(end)
        def _():
            done[rows, :] = mine[rows, :].astype(BF16)

        @pl.when(me == 0)
        def _():
            keep(k).start()

        @pl.when(me == 1)
        def _():
            give(k).start()

    loop(PIECES, step)

    def tail(k):
        trade(k).wait_send()

        @pl.when(jnp.logical_not(end))
        def _():
            hand(k, 0).wait_send()

        @pl.when(me == 0)
        def _():
            keep(k).wait()
            give(k).wait_recv()

        @pl.when(me == 1)
        def _():
            give(k).wait_send()

    loop(PIECES, tail)
    own_out.wait()
    for off in OTHERS:
        cold_from(off).wait_recv()
        cold_to(off).wait_send()


def reduce_rows(hot, cold):
    dma = pltpu.SemaphoreType.DMA
    half = hot.shape[0] // 2
    many = dma((PIECES,))
    dev = dma((N_DEV,))
    return pl.pallas_call(
        reduce_kernel,
        in_specs=[ANY, ANY],
        out_specs=[ANY, ANY],
        out_shape=[shape_of(BF16, *hot.shape), shape_of(cold.dtype, *cold.shape)],
        scratch_shapes=[pltpu.VMEM((half, D), F32)] * 3
        + [pltpu.VMEM((half, D), BF16), pltpu.VMEM(cold.shape[1:], cold.dtype), many, dma, many, many, dev, dev, many, many, many, many],
        compiler_params=params(collective_id=3, has_side_effects=True),
        cost_estimate=cost(8e10, 4e7),
        name="reduce_rows",
    )(hot, cold)


ZROWS = 512


def final_kernel(me_s, own_s, tgt_s, rep_s, hot_ref, cold_ref, out_ref, zero, cold, acc, stage, hot, z_sem, c_sem, h_sem, p_sem):
    me = me_s[0]
    pltpu.make_async_copy(cold_ref, cold, c_sem).start()
    zero[...] = jnp.zeros_like(zero)

    def fill(lo, n):
        return pltpu.make_async_copy(zero.at[pl.ds(0, n), :], out_ref.at[pl.ds(lo, n), :], z_sem)

    spans = []
    lo = HOT
    while lo < ROWS:
        n = min(ZROWS, ROWS - lo)
        spans.append((lo, n))
        lo += n
    for lo, n in spans:
        fill(lo, n).start()

    @pl.when(me == 0)
    def _():
        pltpu.make_async_copy(hot_ref, hot, h_sem).start()

    @pl.when(me != 0)
    def _():
        for lo in range(0, HOT, ZROWS):
            fill(lo, ZROWS).start()

    def clear(b):
        acc[pl.ds(pl.multiple_of(b * LANE, LANE), LANE), :] = jnp.zeros((LANE, D), F32)

    loop(2 * COLD // LANE, clear)

    @pl.when(me == 0)
    def _():
        pltpu.make_async_copy(hot_ref, hot, h_sem).wait()
        pltpu.make_async_copy(hot, out_ref.at[pl.ds(0, HOT), :], h_sem).start()

    pltpu.make_async_copy(cold_ref, cold, c_sem).wait()

    def add(q):
        for u in range(8):
            j = q * 8 + u
            r = tgt_s[lax.shift_right_logical(j, 7), jnp.bitwise_and(j, 127)]
            acc[pl.ds(r, 1), :] += cold[pl.ds(j, 1), :]

    loop(COLD // 8, add)

    def conv(b):
        rows = pl.ds(pl.multiple_of(b * LANE, LANE), LANE)
        stage[rows, :] = acc[rows, :].astype(BF16)

    loop(2 * COLD // LANE, conv)

    for lo, n in spans:
        fill(lo, n).wait()

    @pl.when(me == 0)
    def _():
        pltpu.make_async_copy(hot, out_ref.at[pl.ds(0, HOT), :], h_sem).wait()

    @pl.when(me != 0)
    def _():
        for lo in range(0, HOT, ZROWS):
            fill(lo, ZROWS).wait()

    def pair_copy(j, row):
        return pltpu.make_async_copy(
            stage.at[pl.ds(pl.multiple_of(j * 2, 2), 2), :], out_ref.at[pl.ds(pl.multiple_of(row, 2), 2), :], p_sem
        )

    def put(j, count):
        rep = rep_s[lax.shift_right_logical(j, 7), jnp.bitwise_and(j, 127)]
        s = lax.div(j, CAP)
        row = own_s[s, j - s * CAP]
        go = jnp.logical_and(rep == j, row >= 0)

        @pl.when(go)
        def _():
            pair_copy(j, lax.shift_right_logical(jnp.maximum(row, 0), 1) * 2).start()

        return count + go.astype(I32)

    count = lax.fori_loop(0, COLD, put, jnp.int32(0))

    def drain(j):
        pair_copy(0, 0).wait()

    loop(count, drain)


def final_rows(me, own, tgt, rep, hot, cold):
    dma = pltpu.SemaphoreType.DMA
    return pl.pallas_call(
        final_kernel,
        grid_spec=pltpu.PrefetchScalarGridSpec(
            num_scalar_prefetch=4,
            grid=(1,),
            in_specs=[ANY] * 2,
            out_specs=ANY,
            scratch_shapes=[
                pltpu.VMEM((ZROWS, D), BF16),
                pltpu.VMEM((COLD, D), F32),
                pltpu.VMEM((2 * COLD, D), F32),
                pltpu.VMEM((2 * COLD, D), BF16),
                pltpu.VMEM((HOT, D), BF16),
                dma,
                dma,
                dma,
                dma,
            ],
        ),
        out_shape=shape_of(BF16, ROWS, D),
        compiler_params=params(),
        cost_estimate=cost(4e10, 8e7),
        name="final_rows",
    )(me, own, tgt, rep, hot, cold)


def swap_kernel(same, x_ref, out_ref, own_sem, send_sem, recv_sem):
    me = lax.axis_index("fsdp")
    barrier = pltpu.get_barrier_semaphore()
    for off in OTHERS:
        pl.semaphore_signal(barrier, inc=1, device_id=(lax.rem(me + off, N_DEV),), device_id_type=MESH)
    pl.semaphore_wait(barrier, N_DEV - 1)

    def copy(off):
        dst = lax.rem(me + off, N_DEV)
        return pltpu.make_async_remote_copy(
            src_ref=x_ref.at[0 if same else dst],
            dst_ref=out_ref.at[me],
            send_sem=send_sem.at[off],
            recv_sem=recv_sem.at[off],
            device_id=(dst,),
            device_id_type=MESH,
        )

    def inward(off):
        src = lax.rem(me - off + N_DEV, N_DEV)
        return pltpu.make_async_remote_copy(
            src_ref=x_ref.at[0],
            dst_ref=out_ref.at[src],
            send_sem=send_sem.at[off],
            recv_sem=recv_sem.at[off],
            device_id=(src,),
            device_id_type=MESH,
        )

    for off in OTHERS:
        copy(off).start()
    own = pltpu.make_async_copy(x_ref.at[0 if same else me], out_ref.at[me], own_sem)
    own.start()
    own.wait()
    for off in OTHERS:
        inward(off).wait_recv()
    for off in OTHERS:
        copy(off).wait_send()


def swap_blocks(x, cid):
    dma = pltpu.SemaphoreType.DMA
    return pl.pallas_call(
        functools.partial(swap_kernel, x.shape[0] == 1),
        in_specs=[ANY],
        out_specs=ANY,
        out_shape=jax.ShapeDtypeStruct((N_DEV,) + x.shape[1:], x.dtype),
        scratch_shapes=[dma, dma((N_DEV,)), dma((N_DEV,))],
        compiler_params=params(collective_id=cid, has_side_effects=True),
        name="swap_blocks",
    )(x)


SLOW = LANE


def general_lookup(table, ids, first):
    def step(c, x):
        loc = lax.dynamic_slice(ids, (0, c * SLOW), (N_DEV, SLOW)) - first
        owned = (loc >= 0) & (loc < ROWS)
        rows = jnp.take(table, jnp.where(owned, loc, 0), axis=0)
        rows = jnp.where(owned[..., None], rows, jnp.zeros((), BF16))
        got = swap_blocks(rows, 1).astype(F32).sum(0).astype(BF16)
        return lax.dynamic_update_slice(x, got, (c * SLOW, 0))

    return lax.fori_loop(0, TOK // SLOW, step, jnp.zeros((TOK, D), BF16))


def general_scatter(d_x, ids, first):
    def step(c, acc):
        loc = lax.dynamic_slice(ids, (0, c * SLOW), (N_DEV, SLOW)) - first
        owned = (loc >= 0) & (loc < ROWS)
        got = swap_blocks(lax.dynamic_slice(d_x, (c * SLOW, 0), (SLOW, D))[None], 2)
        seg = jnp.where(owned, loc, ROWS)
        return acc.at[seg.reshape(-1)].add(got.reshape(-1, D), mode="drop")

    acc = lax.fori_loop(0, TOK // SLOW, step, jnp.zeros((ROWS, D), F32))
    return acc.astype(BF16)


def rope_tables():
    half = HEAD_DIM // 2
    inv_freq = jnp.power(ROPE_THETA, -(jnp.arange(half, dtype=F32) * 2.0 / HEAD_DIM))
    angles = jnp.arange(SEQ, dtype=F32)[:, None] * inv_freq[None, :]
    cos_h, sin_h = jnp.cos(angles), jnp.sin(angles)
    return jnp.concatenate([cos_h, cos_h], axis=-1), jnp.concatenate([-sin_h, sin_h], axis=-1)


def device_step(tok_ids, grad_out, table, gain_p, wq_p, bq_p, wk_p, bk_p, wv_p, bv_p, wo_p):
    ax = "fsdp"
    me = lax.axis_index(ax)
    me1 = me.reshape(1).astype(I32)
    first = me * ROWS
    kvw = KV * HEAD_DIM
    w_in = jnp.concatenate([wq_p, wk_p, wv_p], axis=1)
    w_in, wo_p = lax.optimization_barrier((w_in, wo_p))
    w_qkv = lax.all_gather(w_in, ax, axis=0, tiled=True)
    w_out = lax.all_gather(wo_p, ax, axis=0, tiled=True)
    small = [v.astype(F32) for v in (gain_p, bq_p, bk_p, bv_p)]
    size = [v.shape[0] for v in small]
    fill = PACK * LANE - TOK - sum(size)
    pk = jnp.concatenate([tok_ids.astype(F32).reshape(-1)] + small + [jnp.zeros(fill, F32)]).reshape(PACK, LANE)
    hot_rows, every, xi, hid_idx, slot, own, most = prologue(pk, table)
    every = every.reshape(N_DEV, -1)
    ids = every[:, :TOK].astype(I32)
    over = most[0, 0] > CAP
    vecs, at = [], TOK
    for n in size:
        vecs.append(every[:, at : at + n].reshape(1, -1))
        at += n
    gain = vecs[0]
    bias = jnp.concatenate(vecs[1:], axis=1)
    cos_t, sin_t = rope_tables()

    cold_x = lax.all_to_all(gather_rows(table, own, CAP), ax, 0, 0, tiled=True).reshape(COLD, D)
    xh, slot_x = lax.cond(
        over,
        lambda: (general_lookup(table, ids, first), jnp.full_like(slot, -1)),
        lambda: (gather_rows(hot_rows, hid_idx, LANE).reshape(TOK, D), slot),
    )
    go = grad_out.reshape(TOK, D)
    d_attn = dot(go, w_out, NT).astype(BF16)
    x, hid, qkv = proj(xh, slot_x, cold_x, gain, w_qkv, bias, cos_t, sin_t)
    attn, dq, dk, dv, s_q, s_k, s_v = attention(qkv, d_attn, cos_t, sin_t)
    gw_out = dot(attn, go, TN)
    gw_out, dq = lax.optimization_barrier((gw_out, dq))
    g_out = lax.psum_scatter(gw_out, ax, scatter_dimension=0, tiled=True)
    gw_qkv = qkv_weight_grad(hid, dq, dk, dv)
    gw_qkv, dq, dk, dv = lax.optimization_barrier((gw_qkv, dq, dk, dv))
    g_qkv = lax.psum_scatter(gw_qkv, ax, scatter_dimension=0, tiled=True)
    d_x, s_g = input_grad(dq, dk, dv, w_qkv, x, go, gain)
    block_out = (x.astype(F32) + dot(attn, w_out, NN)).astype(BF16).reshape(grad_out.shape)

    parts = [s_g.sum(0), s_q.sum((0, 1)), s_k.sum((0, 1)), s_v.sum((0, 1))]
    vec = jnp.concatenate([p.reshape(N_DEV, -1) for p in parts], axis=1)
    vec = lax.all_to_all(vec, ax, 0, 0, tiled=True).sum(0)

    hot, cold = scatter_rows(xi, d_x)
    hot, cold = reduce_rows(hot, cold.reshape(N_DEV, CAP, D))
    flat = own[:, :CAP].reshape(1, COLD).astype(F32)
    tgt, rep = merge_maps(flat, flat.reshape(COLD, 1))
    grad_table = lax.cond(
        over,
        lambda: general_scatter(d_x, ids, first),
        lambda: final_rows(me1, own, tgt, rep, hot, cold.reshape(COLD, D)),
    )
    cut = [sum(size[:i]) for i in range(len(size) + 1)]
    g_gain, g_bq, g_bk, g_bv = (vec[a:b] for a, b in zip(cut[:-1], cut[1:], strict=True))
    g_q, g_k, g_v = g_qkv[:, :D], g_qkv[:, D : D + kvw], g_qkv[:, D + kvw :]
    return block_out, grad_table, g_gain, g_q, g_bq, g_k, g_bk, g_v, g_bv, g_out


def solution(mesh):
    row = P("fsdp", None)
    vec = P("fsdp")
    act = P("fsdp", None, None)
    weights = (vec, row, vec, row, vec, row, vec, row)
    return jax.shard_map(
        device_step, mesh=mesh, in_specs=(row, act, row) + weights, out_specs=(act, row) + weights, check_vma=False
    )
```
